32 devices in a mesh: dom: 16 (over z, y, core), sub: 2 (over x).
Axes of the slice: x: 2, y: 2, z: 4, core: 2. Of those that a mesh axis runs over, the one named last changes fastest.
Arguments:
- fine_partial: float32 [2, 165, 2048], P('sub', None, 'dom'), may hold values from -6 to 6
- upward_ops: float32 [8, 165, 165], replicated, may hold values from -0.15625 to 0.15625
- interaction_ops: float32 [188, 165, 165], P('sub'), may hold values from -0.03125 to 0.03125
- downward_ops: float32 [8, 165, 165], replicated, may hold values from -0.5 to 0.5
- fine_list: int32 [188, 2048], P('sub', 'dom'), may hold values from -1 to 2047, as said below
- mid_list: int32 [188, 256], P('sub', 'dom'), may hold values from -1 to 255, as said below
- top_list: int32 [188, 32], P('sub', 'dom'), may hold values from -1 to 31, as said below
- upper_list: int32 [188, 4], P('sub'), may hold values from -1 to 3, as said below
- positions: float32 [3, 65536], P(None, ('dom', 'sub')), may hold values from -0.5 to 0.5
- leaf_cell: int32 [65536], P(('dom', 'sub')), may hold values from 0 to 2047, as said below
Outputs:
- local_fine: float32 [165, 2048], P(None, 'dom')
- potential: float32 [65536], P(('dom', 'sub'))
The draws below stay inside these ranges and needn't reach their ends.
Inputs may be any that keep to these rules, and one draw needn't show every extreme that they name: `fine_list`: column t lists for each offset slot a cell of the finest level within 128 cells of t in Peano order, or -1 for an empty slot. `mid_list`: column t lists for each offset slot a cell of the middle level within 16 cells of t, or -1 for an empty slot. `top_list`: each entry is a cell of the top level, or -1 for an empty slot. `upper_list`: each entry is a cell of the upper level, or -1 for an empty slot. `leaf_cell`: A particle's leaf is one of the 128 finest cells owned by its own slab.
All inputs are finite; a program needn't handle non-finite values.
Results may differ from the reference program's by a relative error of at most 0.0003.
Values sent between devices are 32-bit elements; how exact they have to be, the bound alone decides.
A program may use at most 128 MiB of HBM per device.

```python
import jax
import jax.numpy as jnp
from jax import lax

ORDER = 8
NC = 165
NOFF = 188
CF = 128
NF = 2048
NM = 256
NT = 32
NU = 4
PARTICLES = 65536
N_DOM = 16
N_SUB = 2


def window_list(key, cells_total, reach):
    targets = jnp.arange(cells_total, dtype=jnp.int32)[None, :]
    offsets = jax.random.randint(key, (NOFF, cells_total), -reach, reach + 1, dtype=jnp.int32)
    sources = targets + offsets
    inside = (sources >= 0) & (sources < cells_total)
    return jnp.where(inside, sources, -1).astype(jnp.int32)


def global_list(key, cells_total):
    key_one, key_two = jax.random.split(key)
    drawn_cells = jax.random.randint(key_one, (NOFF, cells_total), 0, cells_total, dtype=jnp.int32)
    vacant = jax.random.randint(key_two, (NOFF, cells_total), 0, 8, dtype=jnp.int32) == 0
    return jnp.where(vacant, -1, drawn_cells).astype(jnp.int32)


def draw_fine_list(key, part):
    return window_list(jax.random.fold_in(key, 11), NF, CF)


def draw_mid_list(key, part):
    return window_list(jax.random.fold_in(key, 12), NM, CF // 8)


def draw_top_list(key, part):
    return global_list(jax.random.fold_in(key, 13), NT)


def draw_upper_list(key, part):
    return global_list(jax.random.fold_in(key, 14), NU)


def draw_leaf_cell(key, part):
    slabs = NF // CF
    indices = jnp.arange(PARTICLES, dtype=jnp.int32)
    slab_index = indices // (PARTICLES // slabs)
    inner = jax.random.randint(jax.random.fold_in(key, 15), (PARTICLES,), 0, CF, dtype=jnp.int32)
    return (slab_index * CF + inner).astype(jnp.int32)


def level_of(stream_key, extent, shards, smallest, top_value):
    gain, own = 1.0, jax.random.fold_in(stream_key, 6)
    for position, blocks in shards:
        draws = jnp.exp(jax.random.uniform(jax.random.fold_in(own, position), (blocks,), jnp.float32, smallest / len(shards), top_value / len(shards)))
        gain = gain * jnp.repeat(draws, extent[position] // blocks).reshape([-1 if axis == position else 1 for axis in range(len(extent))])
    return gain


def noise(key, dims, scale, most, pieces=(), kind=jnp.bfloat16):
    result = scale * jax.random.normal(key, dims, jnp.float32)
    if pieces:
        result = result * level_of(key, dims, pieces, -0.22, 0.18)
    return jnp.clip(result, -most, most).astype(kind)


def setup_inputs(seed: int = 0) -> dict:
    splits = jax.random.split(jax.random.key(seed), 11)
    return {
        "fine_partial": noise(splits[0], (N_SUB, NC, NF), 1.0, 6.0, ((0, 2), (2, 16)), jnp.float32),
        "upward_ops": noise(splits[1], (8, NC, NC), (8 * NC) ** -0.5, 0.15625, (), jnp.float32),
        "interaction_ops": noise(splits[2], (NOFF, NC, NC), (NOFF * NC) ** -0.5, 0.03125, ((0, 2),), jnp.float32),
        "downward_ops": noise(splits[3], (8, NC, NC), NC ** -0.5, 0.5, (), jnp.float32),
        "fine_list": draw_fine_list(jax.random.fold_in(splits[10], 71), 0),
        "mid_list": draw_mid_list(jax.random.fold_in(splits[10], 71), 0),
        "top_list": draw_top_list(jax.random.fold_in(splits[10], 71), 0),
        "upper_list": draw_upper_list(jax.random.fold_in(splits[10], 71), 0),
        "positions": jnp.clip(jax.random.uniform(splits[8], (3, PARTICLES), jnp.float32, -0.5, 0.5) * level_of(splits[8], (3, PARTICLES), ((1, 32),), -0.4, 0.0), -0.5, 0.5),
        "leaf_cell": draw_leaf_cell(jax.random.fold_in(splits[10], 71), 0),
    }


precise = lax.Precision.HIGHEST


def exponents():
    entries = []
    for degree in range(ORDER + 1):
        for along_x in range(degree, -1, -1):
            for along_y in range(degree - along_x, -1, -1):
                entries.append((along_x, along_y, degree - along_x - along_y))
    return entries


def monomials(coords):
    powers = [jnp.ones_like(coords)]
    for degree in range(ORDER):
        powers.append(powers[-1] * coords)
    rows = []
    for triple in exponents():
        rows.append(powers[triple[0]][0] * powers[triple[1]][1] * powers[triple[2]][2])
    return jnp.stack(rows)


def upward(moments, upward_ops):
    parents = moments.shape[1] // 8
    grouped = moments.reshape(moments.shape[0], parents, 8)
    return jnp.einsum("oab,bpo->ap", upward_ops, grouped, precision=precise)


def downward(expansions, downward_ops):
    spread = jnp.einsum("oab,bp->apo", downward_ops, expansions, precision=precise)
    return spread.reshape(spread.shape[0], -1)


def interact(moments, sources, interaction_ops, block_size):
    targets = sources.shape[1]

    def one_block(block_index):
        chosen = lax.dynamic_slice_in_dim(sources, block_index * block_size, block_size, 1)
        present = chosen >= 0
        picked = jnp.take(moments, jnp.clip(chosen, 0, moments.shape[1] - 1), axis=1)
        picked = jnp.where(present[None], picked, jnp.float32(0.0))
        return jnp.einsum("jab,bjt->at", interaction_ops, picked, precision=precise)

    results = lax.map(one_block, jnp.arange(targets // block_size, dtype=jnp.int32))
    return jnp.transpose(results, (1, 0, 2)).reshape(moments.shape[0], targets)


def reference(fine_partial, upward_ops, interaction_ops, downward_ops, fine_list, mid_list, top_list, upper_list, positions, leaf_cell):
    fine_moments = jnp.sum(fine_partial, axis=0)
    mid_moments = upward(fine_moments, upward_ops)
    top_moments = upward(mid_moments, upward_ops)
    upper_moments = upward(top_moments, upward_ops)
    local_upper = interact(upper_moments, upper_list, interaction_ops, upper_moments.shape[1])
    local_top = interact(top_moments, top_list, interaction_ops, CF // 64) + downward(local_upper, downward_ops)
    local_mid = interact(mid_moments, mid_list, interaction_ops, CF // 8) + downward(local_top, downward_ops)
    local_fine = interact(fine_moments, fine_list, interaction_ops, CF) + downward(local_mid, downward_ops)
    slab_span = PARTICLES // N_DOM

    def slab_potential(slab_index):
        coords = lax.dynamic_slice_in_dim(positions, slab_index * slab_span, slab_span, 1)
        leaves = lax.dynamic_slice_in_dim(leaf_cell, slab_index * slab_span, slab_span, 0)
        columns = jnp.take(local_fine, leaves, axis=1)
        return jnp.sum(columns * monomials(coords), axis=0)

    potential = lax.map(slab_potential, jnp.arange(N_DOM, dtype=jnp.int32)).reshape(-1)
    return local_fine, potential
```

```python
import functools

import jax
import jax.numpy as jnp
from jax import lax
from jax.experimental import pallas as pl
from jax.experimental.pallas import tpu as pltpu
from jax.sharding import PartitionSpec as P

ORDER = 8
LANES = 128


precise = lax.Precision.HIGHEST


def round_up(count, unit):
    return -(-count // unit) * unit


def exponents():
    entries = []
    for degree in range(ORDER + 1):
        for along_x in range(degree, -1, -1):
            for along_y in range(degree - along_x, -1, -1):
                entries.append((along_x, along_y, degree - along_x - along_y))
    return entries


def halves(value):
    high = value.astype(jnp.bfloat16)
    low = (value - high.astype(jnp.float32)).astype(jnp.bfloat16)
    return high, low


def one_hot(row, count):
    places = lax.broadcasted_iota(jnp.int32, (count, row.shape[1]), 0)
    return jnp.where(places == row, 1.0, 0.0).astype(jnp.bfloat16)


def interact_kernel(
    coeffs, slots, group, fine_ref, coarse_ref, fine_list, coarse_list, ops_ref, out_ref,
    fine_table, coarse_table, fine_picked, coarse_picked,
):
    rows = fine_ref.shape[0]
    depth = fine_list.shape[0]
    step = pl.program_id(0)

    @pl.when(step == 0)
    def _():
        for source, table in ((fine_ref, fine_table), (coarse_ref, coarse_table)):
            high, low = halves(source[...])
            table[...] = jnp.concatenate([high, low], axis=0)

        def pick(pair, carry):
            for table, entries, picked in (
                (fine_table, fine_list, fine_picked),
                (coarse_table, coarse_list, coarse_picked),
            ):
                chosen = jnp.concatenate(
                    [
                        one_hot(entries[pl.ds(2 * pair + k, 1), :], table.shape[1])
                        for k in range(2)
                    ],
                    axis=1,
                )
                both = jnp.dot(table[...], chosen, preferred_element_type=jnp.float32)
                value = both[:rows] + both[rows:]
                for k in range(2):
                    picked[pl.ds(2 * pair + k, rows, stride=depth), :] = value[
                        :, k * LANES : (k + 1) * LANES
                    ]
            return carry

        lax.fori_loop(0, depth // 2, pick, 0)
        out_ref[...] = jnp.zeros_like(out_ref)

    lane = lax.broadcasted_iota(jnp.int32, (rows, LANES), 1)
    filler = jnp.zeros((LANES - depth, 2 * LANES), jnp.bfloat16)
    for part in range(group // 8):
        block = jnp.swapaxes(ops_ref[:, 8 * part : 8 * part + 8, :], 0, 1)
        left = []
        right = []
        for k in range(8):
            term = step * group + 8 * part + k
            op = jnp.where((lane < slots) & (term < coeffs), block[k], 0.0)
            op_high, op_low = halves(op)
            start = pl.multiple_of(term * depth, 8)
            data = jnp.concatenate(
                [
                    fine_picked[pl.ds(start, depth), :],
                    coarse_picked[pl.ds(start, depth), :],
                ],
                axis=1,
            )
            high, low = halves(data)
            high = jnp.concatenate([high, filler], axis=0)
            low = jnp.concatenate([low, filler], axis=0)
            left += [op_high, op_high, op_low]
            right += [high, low, high]
        out_ref[...] += jnp.dot(
            jnp.concatenate(left, axis=1),
            jnp.concatenate(right, axis=0),
            preferred_element_type=jnp.float32,
        )


def interact(fine, coarse, fine_list, coarse_list, ops):
    coeffs, _, slots = ops.shape
    rows, width = fine.shape
    coarse_width = coarse.shape[1]
    depth = fine_list.shape[0]
    group = 24
    whole = lambda array: pl.BlockSpec(array.shape, lambda i: (0, 0))
    return pl.pallas_call(
        functools.partial(interact_kernel, coeffs, slots, group),
        grid=(rows // group,),
        in_specs=[
            whole(fine),
            whole(coarse),
            whole(fine_list),
            whole(coarse_list),
            pl.BlockSpec((rows, group, LANES), lambda i: (0, i, 0)),
        ],
        out_specs=pl.BlockSpec((rows, 2 * LANES), lambda i: (0, 0)),
        out_shape=jax.ShapeDtypeStruct((rows, 2 * LANES), jnp.float32),
        scratch_shapes=[
            pltpu.VMEM((2 * rows, width), jnp.bfloat16),
            pltpu.VMEM((2 * rows, coarse_width), jnp.bfloat16),
            pltpu.VMEM((rows * depth, LANES), jnp.float32),
            pltpu.VMEM((rows * depth, LANES), jnp.float32),
        ],
        compiler_params=pltpu.CompilerParams(vmem_limit_bytes=48 * 1024 * 1024),
        cost_estimate=pl.CostEstimate(
            flops=6 * rows * rows * LANES * 2 * LANES,
            bytes_accessed=4 * rows * rows * LANES,
            transcendentals=0,
        ),
    )(fine, coarse, fine_list, coarse_list, ops)


def potential_kernel(local_ref, leaf_ref, position_ref, exponent_ref, out_ref):
    rows, cells = local_ref.shape
    particles = leaf_ref.shape[1]
    high, low = halves(local_ref[...])
    table = jnp.concatenate([high, low], axis=0)
    masks = [
        [(exponent_ref[:, axis : axis + 1] // bit) % 2 == 1 for bit in (1, 2, 4, 8)]
        for axis in range(3)
    ]
    for start in range(0, particles, 2 * LANES):
        span = slice(start, start + 2 * LANES)
        chosen = one_hot(leaf_ref[:, span], cells)
        both = jnp.dot(table, chosen, preferred_element_type=jnp.float32)
        value = both[:rows] + both[rows:]
        for axis in range(3):
            power = position_ref[axis : axis + 1, span]
            for bit in range(4):
                value = value * jnp.where(masks[axis][bit], power, 1.0)
                power = power * power
        out_ref[:, span] = jnp.sum(value, axis=0, keepdims=True)


def evaluate(local, leaves, positions):
    rows = local.shape[0]
    table = jnp.asarray(exponents(), jnp.int32)
    table = jnp.pad(table, ((0, rows - table.shape[0]), (0, LANES - 3)))
    return pl.pallas_call(
        potential_kernel,
        out_shape=jax.ShapeDtypeStruct((1, leaves.shape[0]), jnp.float32),
        compiler_params=pltpu.CompilerParams(vmem_limit_bytes=32 * 1024 * 1024),
    )(local, leaves[None], positions, table)[0]


def upward(moments, upward_ops):
    parents = moments.shape[1] // 8
    grouped = moments.reshape(moments.shape[0], parents, 8)
    return jnp.einsum("oab,bpo->ap", upward_ops, grouped, precision=precise)


def downward(expansions, downward_ops):
    spread = jnp.einsum("oab,bp->apo", downward_ops, expansions, precision=precise)
    return spread.reshape(spread.shape[0], -1)


def settle(portion):
    count = lax.axis_size("sub")
    ring = [(i, (i + 1) % count) for i in range(count)]
    total = moving = portion
    for _ in range(count - 1):
        moving = lax.ppermute(moving, "sub", ring)
        total = total + moving
    return total


def extended(block):
    count = lax.axis_size("dom")
    forward = [(i, i + 1) for i in range(count - 1)]
    backward = [(target, source) for source, target in forward]
    low = lax.ppermute(block, "dom", forward)
    high = lax.ppermute(block, "dom", backward)
    return jnp.concatenate([low, block, high], axis=1)


def shards(
    fine_partial,
    upward_ops,
    interaction_ops,
    downward_ops,
    fine_list,
    mid_list,
    top_list,
    upper_list,
    positions,
    leaf_cell,
):
    slab_cells = fine_partial.shape[2]
    mid_cells = slab_cells // 8
    top_cells = slab_cells // 64
    domain = lax.axis_index("dom")
    slots, coeffs = interaction_ops.shape[:2]
    rows = round_up(coeffs, 24)
    depth = round_up(slots, 16)
    upper_span = max(1, top_cells // 8)
    upper_first = domain * top_cells // 8
    upper_sources = lax.dynamic_slice_in_dim(upper_list, upper_first, upper_span, 1)

    wide_fine = extended(settle(fine_partial[0]))
    wide_mid = upward(wide_fine, upward_ops)
    own_top = upward(wide_mid[:, mid_cells : 2 * mid_cells], upward_ops)
    top_moments = lax.all_gather(own_top, "dom", axis=1, tiled=True)
    upper_moments = upward(top_moments, upward_ops)

    def place(sources, offset):
        return jnp.where(sources >= 0, sources + offset, -1)

    def padded(array, height, width, fill):
        return jnp.pad(
            array,
            ((0, height - array.shape[0]), (0, width - array.shape[1])),
            constant_values=fill,
        )

    spread = wide_mid.shape[1]
    coarse = jnp.concatenate([wide_mid, top_moments, upper_moments], axis=1)
    coarse_sources = jnp.concatenate(
        [
            place(mid_list, mid_cells - domain * mid_cells),
            place(top_list, spread),
            place(upper_sources, spread + top_moments.shape[1]),
        ],
        axis=1,
    )
    fine_sources = place(fine_list, slab_cells - domain * slab_cells)
    terms = interact(
        padded(wide_fine, rows, wide_fine.shape[1], 0),
        padded(coarse, rows, round_up(coarse.shape[1], LANES), 0),
        padded(fine_sources, depth, LANES, -1),
        padded(coarse_sources, depth, LANES, -1),
        jnp.transpose(interaction_ops, (1, 2, 0)),
    )
    terms = settle(terms)[:coeffs]
    at = LANES
    mid_term = terms[:, at : at + mid_cells]
    at += mid_cells
    top_term = terms[:, at : at + top_cells]
    at += top_cells
    local_upper = terms[:, at : at + upper_span]
    down_top = downward(local_upper, downward_ops)
    top_offset = domain * top_cells % 8
    local_top = top_term + lax.dynamic_slice_in_dim(down_top, top_offset, top_cells, 1)
    local_mid = mid_term + downward(local_top, downward_ops)
    local_fine = terms[:, :slab_cells] + downward(local_mid, downward_ops)
    potential = evaluate(
        padded(local_fine, rows, slab_cells, 0), leaf_cell - domain * slab_cells, positions
    )
    return (local_fine, potential)


def solution(mesh):
    placed = (
        P("sub", None, "dom"),
        P(),
        P("sub", None, None),
        P(),
        P("sub", "dom"),
        P("sub", "dom"),
        P("sub", "dom"),
        P("sub", None),
        P(None, ("dom", "sub")),
        P(("dom", "sub")),
    )
    return jax.shard_map(
        shards,
        mesh=mesh,
        in_specs=placed,
        out_specs=(P(None, "dom"), P(("dom", "sub"))),
        check_vma=False,
    )
```

```python
import functools

import jax
import jax.numpy as jnp
from jax import lax
from jax.experimental import pallas as pl
from jax.experimental.pallas import tpu as pltpu
from jax.sharding import PartitionSpec as P

ORDER = 8
LANES = 128


precise = lax.Precision.HIGHEST


def round_up(count, unit):
    return -(-count // unit) * unit


def exponents():
    entries = []
    for degree in range(ORDER + 1):
        for along_x in range(degree, -1, -1):
            for along_y in range(degree - along_x, -1, -1):
                entries.append((along_x, along_y, degree - along_x - along_y))
    return entries


def halves(value):
    high = value.astype(jnp.bfloat16)
    low = (value - high.astype(jnp.float32)).astype(jnp.bfloat16)
    return high, low


def one_hot(row, count):
    places = lax.broadcasted_iota(jnp.int32, (count, row.shape[1]), 0)
    return jnp.where(places == row, 1.0, 0.0).astype(jnp.bfloat16)


def interact_kernel(
    coeffs, slots, group, fine_ref, coarse_ref, fine_list, coarse_list, ops_ref, out_ref,
    fine_table, coarse_table, fine_picked, coarse_picked,
):
    rows = fine_ref.shape[0]
    depth = fine_list.shape[0]
    step = pl.program_id(0)

    @pl.when(step == 0)
    def _():
        for source, table in ((fine_ref, fine_table), (coarse_ref, coarse_table)):
            high, low = halves(source[...])
            table[...] = jnp.concatenate([high, low], axis=0)

        def pick(batch, carry):
            base = pl.multiple_of(8 * batch, 8)
            for table, entries, picked in (
                (fine_table, fine_list, fine_picked),
                (coarse_table, coarse_list, coarse_picked),
            ):
                columns = []
                for k in range(0, 8, 2):
                    chosen = jnp.concatenate(
                        [
                            one_hot(entries[pl.ds(base + k + m, 1), :], table.shape[1])
                            for m in range(2)
                        ],
                        axis=1,
                    )
                    both = jnp.dot(table[...], chosen, preferred_element_type=jnp.float32)
                    value = both[:rows] + both[rows:]
                    columns += [value[:, :LANES], value[:, LANES:]]
                picked[:, pl.ds(base, 8), :] = jnp.swapaxes(jnp.stack(columns), 0, 1)
            return carry

        lax.fori_loop(0, depth // 8, pick, 0)
        out_ref[...] = jnp.zeros_like(out_ref)

    lane = lax.broadcasted_iota(jnp.int32, (rows, LANES), 1)
    filler = jnp.zeros((LANES - depth, 2 * LANES), jnp.bfloat16)
    for part in range(group // 8):
        block = jnp.swapaxes(ops_ref[:, 8 * part : 8 * part + 8, :], 0, 1)
        left = []
        right = []
        for k in range(8):
            term = step * group + 8 * part + k
            op = jnp.where((lane < slots) & (term < coeffs), block[k], 0.0)
            op_high, op_low = halves(op)
            data = jnp.concatenate([fine_picked[term], coarse_picked[term]], axis=1)
            high, low = halves(data)
            high = jnp.concatenate([high, filler], axis=0)
            low = jnp.concatenate([low, filler], axis=0)
            left += [op_high, op_high, op_low]
            right += [high, low, high]
        out_ref[...] += jnp.dot(
            jnp.concatenate(left, axis=1),
            jnp.concatenate(right, axis=0),
            preferred_element_type=jnp.float32,
        )


def interact(fine, coarse, fine_list, coarse_list, ops):
    coeffs, _, slots = ops.shape
    rows, width = fine.shape
    coarse_width = coarse.shape[1]
    depth = fine_list.shape[0]
    group = 24
    whole = lambda array: pl.BlockSpec(array.shape, lambda i: (0, 0))
    return pl.pallas_call(
        functools.partial(interact_kernel, coeffs, slots, group),
        grid=(rows // group,),
        in_specs=[
            whole(fine),
            whole(coarse),
            whole(fine_list),
            whole(coarse_list),
            pl.BlockSpec((rows, group, LANES), lambda i: (0, i, 0)),
        ],
        out_specs=pl.BlockSpec((rows, 2 * LANES), lambda i: (0, 0)),
        out_shape=jax.ShapeDtypeStruct((rows, 2 * LANES), jnp.float32),
        scratch_shapes=[
            pltpu.VMEM((2 * rows, width), jnp.bfloat16),
            pltpu.VMEM((2 * rows, coarse_width), jnp.bfloat16),
            pltpu.VMEM((rows, depth, LANES), jnp.float32),
            pltpu.VMEM((rows, depth, LANES), jnp.float32),
        ],
        compiler_params=pltpu.CompilerParams(vmem_limit_bytes=48 * 1024 * 1024),
        cost_estimate=pl.CostEstimate(
            flops=6 * rows * rows * LANES * 2 * LANES,
            bytes_accessed=4 * rows * rows * LANES,
            transcendentals=0,
        ),
    )(fine, coarse, fine_list, coarse_list, ops)


def potential_kernel(local_ref, leaf_ref, position_ref, exponent_ref, out_ref):
    rows, cells = local_ref.shape
    particles = leaf_ref.shape[1]
    high, low = halves(local_ref[...])
    table = jnp.concatenate([high, low], axis=0)
    masks = [
        [(exponent_ref[:, axis : axis + 1] // bit) % 2 == 1 for bit in (1, 2, 4, 8)]
        for axis in range(3)
    ]
    for start in range(0, particles, 2 * LANES):
        span = slice(start, start + 2 * LANES)
        chosen = one_hot(leaf_ref[:, span], cells)
        both = jnp.dot(table, chosen, preferred_element_type=jnp.float32)
        value = both[:rows] + both[rows:]
        for axis in range(3):
            power = position_ref[axis : axis + 1, span]
            for bit in range(4):
                value = value * jnp.where(masks[axis][bit], power, 1.0)
                power = power * power
        out_ref[:, span] = jnp.sum(value, axis=0, keepdims=True)


def evaluate(local, leaves, positions):
    rows = local.shape[0]
    table = jnp.asarray(exponents(), jnp.int32)
    table = jnp.pad(table, ((0, rows - table.shape[0]), (0, LANES - 3)))
    return pl.pallas_call(
        potential_kernel,
        out_shape=jax.ShapeDtypeStruct((1, leaves.shape[0]), jnp.float32),
        compiler_params=pltpu.CompilerParams(vmem_limit_bytes=32 * 1024 * 1024),
    )(local, leaves[None], positions, table)[0]


def upward(moments, upward_ops):
    parents = moments.shape[1] // 8
    grouped = moments.reshape(moments.shape[0], parents, 8)
    return jnp.einsum("oab,bpo->ap", upward_ops, grouped, precision=precise)


def downward(expansions, downward_ops):
    spread = jnp.einsum("oab,bp->apo", downward_ops, expansions, precision=precise)
    return spread.reshape(spread.shape[0], -1)


def settle(portion):
    count = lax.axis_size("sub")
    ring = [(i, (i + 1) % count) for i in range(count)]
    total = moving = portion
    for _ in range(count - 1):
        moving = lax.ppermute(moving, "sub", ring)
        total = total + moving
    return total


def extended(block):
    count = lax.axis_size("dom")
    forward = [(i, i + 1) for i in range(count - 1)]
    backward = [(target, source) for source, target in forward]
    low = lax.ppermute(block, "dom", forward)
    high = lax.ppermute(block, "dom", backward)
    return jnp.concatenate([low, block, high], axis=1)


def shards(
    fine_partial,
    upward_ops,
    interaction_ops,
    downward_ops,
    fine_list,
    mid_list,
    top_list,
    upper_list,
    positions,
    leaf_cell,
):
    slab_cells = fine_partial.shape[2]
    mid_cells = slab_cells // 8
    top_cells = slab_cells // 64
    domain = lax.axis_index("dom")
    slots, coeffs = interaction_ops.shape[:2]
    rows = round_up(coeffs, 24)
    depth = round_up(slots, 16)
    upper_span = max(1, top_cells // 8)
    upper_first = domain * top_cells // 8
    upper_sources = lax.dynamic_slice_in_dim(upper_list, upper_first, upper_span, 1)

    wide_fine = extended(settle(fine_partial[0]))
    wide_mid = upward(wide_fine, upward_ops)
    own_top = upward(wide_mid[:, mid_cells : 2 * mid_cells], upward_ops)
    top_moments = lax.all_gather(own_top, "dom", axis=1, tiled=True)
    upper_moments = upward(top_moments, upward_ops)

    def place(sources, offset):
        return jnp.where(sources >= 0, sources + offset, -1)

    def padded(array, height, width, fill):
        return jnp.pad(
            array,
            ((0, height - array.shape[0]), (0, width - array.shape[1])),
            constant_values=fill,
        )

    spread = wide_mid.shape[1]
    coarse = jnp.concatenate([wide_mid, top_moments, upper_moments], axis=1)
    coarse_sources = jnp.concatenate(
        [
            place(mid_list, mid_cells - domain * mid_cells),
            place(top_list, spread),
            place(upper_sources, spread + top_moments.shape[1]),
        ],
        axis=1,
    )
    fine_sources = place(fine_list, slab_cells - domain * slab_cells)
    terms = interact(
        padded(wide_fine, rows, wide_fine.shape[1], 0),
        padded(coarse, rows, round_up(coarse.shape[1], LANES), 0),
        padded(fine_sources, depth, LANES, -1),
        padded(coarse_sources, depth, LANES, -1),
        jnp.transpose(interaction_ops, (1, 2, 0)),
    )
    terms = settle(terms)[:coeffs]
    at = LANES
    mid_term = terms[:, at : at + mid_cells]
    at += mid_cells
    top_term = terms[:, at : at + top_cells]
    at += top_cells
    local_upper = terms[:, at : at + upper_span]
    down_top = downward(local_upper, downward_ops)
    top_offset = domain * top_cells % 8
    local_top = top_term + lax.dynamic_slice_in_dim(down_top, top_offset, top_cells, 1)
    local_mid = mid_term + downward(local_top, downward_ops)
    local_fine = terms[:, :slab_cells] + downward(local_mid, downward_ops)
    potential = evaluate(
        padded(local_fine, rows, slab_cells, 0), leaf_cell - domain * slab_cells, positions
    )
    return (local_fine, potential)


def solution(mesh):
    placed = (
        P("sub", None, "dom"),
        P(),
        P("sub", None, None),
        P(),
        P("sub", "dom"),
        P("sub", "dom"),
        P("sub", "dom"),
        P("sub", None),
        P(None, ("dom", "sub")),
        P(("dom", "sub")),
    )
    return jax.shard_map(
        shards,
        mesh=mesh,
        in_specs=placed,
        out_specs=(P(None, "dom"), P(("dom", "sub"))),
        check_vma=False,
    )
```

```python
import functools

import jax
import jax.numpy as jnp
from jax import lax
from jax.experimental import pallas as pl
from jax.experimental.pallas import tpu as pltpu
from jax.sharding import PartitionSpec as P

ORDER = 8
LANES = 128


precise = lax.Precision.HIGHEST


def round_up(count, unit):
    return -(-count // unit) * unit


def exponents():
    entries = []
    for degree in range(ORDER + 1):
        for along_x in range(degree, -1, -1):
            for along_y in range(degree - along_x, -1, -1):
                entries.append((along_x, along_y, degree - along_x - along_y))
    return entries


def halves(value):
    high = value.astype(jnp.bfloat16)
    low = (value - high.astype(jnp.float32)).astype(jnp.bfloat16)
    return high, low


def one_hot(row, count):
    places = lax.broadcasted_iota(jnp.int32, (count, row.shape[1]), 0)
    return jnp.where(places == row, 1.0, 0.0).astype(jnp.bfloat16)


def interact_kernel(
    coeffs, slots, group, fine_ref, coarse_ref, fine_list, coarse_list, ops_ref, out_ref,
    fine_table, coarse_table, fine_picked, coarse_picked,
):
    rows = fine_ref.shape[0]
    depth = fine_list.shape[0]
    step = pl.program_id(0)

    @pl.when(step == 0)
    def _():
        for source, table in ((fine_ref, fine_table), (coarse_ref, coarse_table)):
            high, low = halves(source[...])
            table[...] = jnp.concatenate([high, low], axis=0)

        def pick(batch, carry):
            base = pl.multiple_of(8 * batch, 8)
            for table, entries, picked in (
                (fine_table, fine_list, fine_picked),
                (coarse_table, coarse_list, coarse_picked),
            ):
                columns = []
                for k in range(0, 8, 2):
                    chosen = jnp.concatenate(
                        [
                            one_hot(entries[pl.ds(base + k + m, 1), :], table.shape[1])
                            for m in range(2)
                        ],
                        axis=1,
                    )
                    both = jnp.dot(table[...], chosen, preferred_element_type=jnp.float32)
                    value = both[:rows] + both[rows:]
                    columns += [value[:, :LANES], value[:, LANES:]]
                picked[:, pl.ds(base, 8), :] = jnp.swapaxes(jnp.stack(columns), 0, 1)
            return carry

        lax.fori_loop(0, depth // 8, pick, 0)
        out_ref[...] = jnp.zeros_like(out_ref)

    lane = lax.broadcasted_iota(jnp.int32, (rows, LANES), 1)
    filler = jnp.zeros((LANES - depth, 2 * LANES), jnp.bfloat16)
    for part in range(group // 8):
        block = jnp.swapaxes(ops_ref[:, 8 * part : 8 * part + 8, :], 0, 1)
        left = []
        right = []
        for k in range(8):
            term = step * group + 8 * part + k
            op = jnp.where((lane < slots) & (term < coeffs), block[k], 0.0)
            op_high, op_low = halves(op)
            data = jnp.concatenate([fine_picked[term], coarse_picked[term]], axis=1)
            high, low = halves(data)
            high = jnp.concatenate([high, filler], axis=0)
            low = jnp.concatenate([low, filler], axis=0)
            left += [op_high, op_high, op_low]
            right += [high, low, high]
        out_ref[...] += jnp.dot(
            jnp.concatenate(left, axis=1),
            jnp.concatenate(right, axis=0),
            preferred_element_type=jnp.float32,
        )


def interact(fine, coarse, fine_list, coarse_list, ops):
    coeffs, _, slots = ops.shape
    rows, width = fine.shape
    coarse_width = coarse.shape[1]
    depth = fine_list.shape[0]
    group = 24
    whole = lambda array: pl.BlockSpec(array.shape, lambda i: (0, 0))
    return pl.pallas_call(
        functools.partial(interact_kernel, coeffs, slots, group),
        grid=(rows // group,),
        in_specs=[
            whole(fine),
            whole(coarse),
            whole(fine_list),
            whole(coarse_list),
            pl.BlockSpec((rows, group, LANES), lambda i: (0, i, 0)),
        ],
        out_specs=pl.BlockSpec((rows, 2 * LANES), lambda i: (0, 0)),
        out_shape=jax.ShapeDtypeStruct((rows, 2 * LANES), jnp.float32),
        scratch_shapes=[
            pltpu.VMEM((2 * rows, width), jnp.bfloat16),
            pltpu.VMEM((2 * rows, coarse_width), jnp.bfloat16),
            pltpu.VMEM((rows, depth, LANES), jnp.float32),
            pltpu.VMEM((rows, depth, LANES), jnp.float32),
        ],
        compiler_params=pltpu.CompilerParams(vmem_limit_bytes=48 * 1024 * 1024),
        cost_estimate=pl.CostEstimate(
            flops=6 * rows * rows * LANES * 2 * LANES,
            bytes_accessed=4 * rows * rows * LANES,
            transcendentals=0,
        ),
    )(fine, coarse, fine_list, coarse_list, ops)


def potential_kernel(local_ref, leaf_ref, position_ref, exponent_ref, out_ref):
    rows, cells = local_ref.shape
    particles = leaf_ref.shape[1]
    high, low = halves(local_ref[...])
    table = jnp.concatenate([high, low], axis=0)
    masks = [
        [(exponent_ref[:, axis : axis + 1] // bit) % 2 == 1 for bit in (1, 2, 4, 8)]
        for axis in range(3)
    ]
    for start in range(0, particles, 2 * LANES):
        span = slice(start, start + 2 * LANES)
        chosen = one_hot(leaf_ref[:, span], cells)
        both = jnp.dot(table, chosen, preferred_element_type=jnp.float32)
        value = both[:rows] + both[rows:]
        for axis in range(3):
            power = position_ref[axis : axis + 1, span]
            for bit in range(4):
                value = value * jnp.where(masks[axis][bit], power, 1.0)
                power = power * power
        out_ref[:, span] = jnp.sum(value, axis=0, keepdims=True)


def evaluate(local, leaves, positions):
    rows = local.shape[0]
    table = jnp.asarray(exponents(), jnp.int32)
    table = jnp.pad(table, ((0, rows - table.shape[0]), (0, LANES - 3)))
    return pl.pallas_call(
        potential_kernel,
        out_shape=jax.ShapeDtypeStruct((1, leaves.shape[0]), jnp.float32),
        compiler_params=pltpu.CompilerParams(vmem_limit_bytes=32 * 1024 * 1024),
    )(local, leaves[None], positions, table)[0]


def exchange_kernel(
    domains, subs, block_ref, top_ref, low_out, high_out, tops_out,
    low, high, tops, side_send, side_recv, top_send, top_recv, own_sem,
):
    domain, sub = lax.axis_index("dom"), lax.axis_index("sub")
    count = domains * subs
    flat = domain * subs + sub
    mesh = pl.DeviceIdType.MESH

    def peer(offset):
        place = lax.rem(flat + offset, count)
        return {"dom": place // subs, "sub": lax.rem(place, subs)}

    barrier = pltpu.get_barrier_semaphore()

    def greet(offset, carry):
        pl.semaphore_signal(barrier, inc=1, device_id=peer(offset), device_id_type=mesh)
        return carry

    lax.fori_loop(1, count, greet, 0)
    own = pltpu.make_async_copy(top_ref, tops.at[count - 1], own_sem)
    own.start()
    pl.semaphore_wait(barrier, count - 1)

    def send(offset, carry):
        pltpu.make_async_remote_copy(
            src_ref=top_ref,
            dst_ref=tops.at[offset - 1],
            send_sem=top_send,
            recv_sem=top_recv,
            device_id=peer(offset),
            device_id_type=mesh,
        ).start()
        return carry

    sides = []
    for index, (target, move) in enumerate(((low, 1), (high, domains - 1))):
        side = pltpu.make_async_remote_copy(
            src_ref=block_ref,
            dst_ref=target,
            send_sem=side_send.at[index],
            recv_sem=side_recv.at[index],
            device_id={"dom": lax.rem(domain + move, domains), "sub": sub},
            device_id_type=mesh,
        )
        side.start()
        sides.append(side)
    lax.fori_loop(1, count, send, 0)
    own.wait()
    arrived = tops.at[pl.ds(0, count - 1)]
    pltpu.make_async_copy(arrived, arrived, top_recv).wait()
    tops_out[...] = jnp.zeros_like(tops_out)

    def gather(offset, carry):
        source = lax.rem(flat + count - offset, count) // subs
        tops_out[source] = tops_out[source] + tops[lax.rem(offset + count - 1, count)]
        return carry

    lax.fori_loop(0, count, gather, 0)
    for side in sides:
        side.wait()
    low_out[...] = low[...]
    high_out[...] = high[...]
    pltpu.make_async_copy(arrived, arrived, top_send).wait()


def exchange(block, top_rows):
    domains, subs = lax.axis_size("dom"), lax.axis_size("sub")
    vmem = pl.BlockSpec(memory_space=pltpu.VMEM)
    return pl.pallas_call(
        functools.partial(exchange_kernel, domains, subs),
        in_specs=[vmem, vmem],
        out_specs=[vmem] * 3,
        out_shape=[
            jax.ShapeDtypeStruct(block.shape, jnp.float32),
            jax.ShapeDtypeStruct(block.shape, jnp.float32),
            jax.ShapeDtypeStruct((domains,) + top_rows.shape, jnp.float32),
        ],
        scratch_shapes=[
            pltpu.VMEM(block.shape, jnp.float32),
            pltpu.VMEM(block.shape, jnp.float32),
            pltpu.VMEM((domains * subs,) + top_rows.shape, jnp.float32),
            pltpu.SemaphoreType.DMA((2,)),
            pltpu.SemaphoreType.DMA((2,)),
            pltpu.SemaphoreType.DMA,
            pltpu.SemaphoreType.DMA,
            pltpu.SemaphoreType.DMA,
        ],
        compiler_params=pltpu.CompilerParams(collective_id=0, has_side_effects=True),
    )(block, top_rows)


def upward(moments, upward_ops):
    parents = moments.shape[1] // 8
    grouped = moments.reshape(moments.shape[0], parents, 8)
    return jnp.einsum("oab,bpo->ap", upward_ops, grouped, precision=precise)


def downward(expansions, downward_ops):
    spread = jnp.einsum("oab,bp->apo", downward_ops, expansions, precision=precise)
    return spread.reshape(spread.shape[0], -1)


def settle(portion):
    count = lax.axis_size("sub")
    ring = [(i, (i + 1) % count) for i in range(count)]
    total = moving = portion
    for _ in range(count - 1):
        moving = lax.ppermute(moving, "sub", ring)
        total = total + moving
    return total


def shards(
    fine_partial,
    upward_ops,
    interaction_ops,
    downward_ops,
    fine_list,
    mid_list,
    top_list,
    upper_list,
    positions,
    leaf_cell,
):
    slab_cells = fine_partial.shape[2]
    mid_cells = slab_cells // 8
    top_cells = slab_cells // 64
    domain = lax.axis_index("dom")
    slots, coeffs = interaction_ops.shape[:2]
    rows = round_up(coeffs, 24)
    depth = round_up(slots, 16)
    upper_span = max(1, top_cells // 8)
    upper_first = domain * top_cells // 8
    upper_sources = lax.dynamic_slice_in_dim(upper_list, upper_first, upper_span, 1)

    partial = fine_partial[0]
    own_top = upward(upward(partial, upward_ops), upward_ops)
    top_rows = jnp.pad(jnp.transpose(own_top), ((0, 0), (0, 2 * LANES - coeffs)))
    block = jnp.pad(settle(partial), ((0, rows - coeffs), (0, 0)))
    low, high, tops = exchange(block, top_rows)
    wide_fine = jnp.concatenate([low, block, high], axis=1)
    wide_mid = upward(wide_fine[:coeffs], upward_ops)
    top_moments = jnp.transpose(tops.reshape(-1, 2 * LANES)[:, :coeffs])
    upper_moments = upward(top_moments, upward_ops)

    def place(sources, offset):
        return jnp.where(sources >= 0, sources + offset, -1)

    def padded(array, height, width, fill):
        return jnp.pad(
            array,
            ((0, height - array.shape[0]), (0, width - array.shape[1])),
            constant_values=fill,
        )

    spread = wide_mid.shape[1]
    coarse = jnp.concatenate([wide_mid, top_moments, upper_moments], axis=1)
    coarse_sources = jnp.concatenate(
        [
            place(mid_list, mid_cells - domain * mid_cells),
            place(top_list, spread),
            place(upper_sources, spread + top_moments.shape[1]),
        ],
        axis=1,
    )
    fine_sources = place(fine_list, slab_cells - domain * slab_cells)
    terms = interact(
        wide_fine,
        padded(coarse, rows, round_up(coarse.shape[1], LANES), 0),
        padded(fine_sources, depth, LANES, -1),
        padded(coarse_sources, depth, LANES, -1),
        jnp.transpose(interaction_ops, (1, 2, 0)),
    )
    terms = settle(terms)[:coeffs]
    at = LANES
    mid_term = terms[:, at : at + mid_cells]
    at += mid_cells
    top_term = terms[:, at : at + top_cells]
    at += top_cells
    local_upper = terms[:, at : at + upper_span]
    down_top = downward(local_upper, downward_ops)
    top_offset = domain * top_cells % 8
    local_top = top_term + lax.dynamic_slice_in_dim(down_top, top_offset, top_cells, 1)
    local_mid = mid_term + downward(local_top, downward_ops)
    local_fine = terms[:, :slab_cells] + downward(local_mid, downward_ops)
    potential = evaluate(
        padded(local_fine, rows, slab_cells, 0), leaf_cell - domain * slab_cells, positions
    )
    return (local_fine, potential)


def solution(mesh):
    placed = (
        P("sub", None, "dom"),
        P(),
        P("sub", None, None),
        P(),
        P("sub", "dom"),
        P("sub", "dom"),
        P("sub", "dom"),
        P("sub", None),
        P(None, ("dom", "sub")),
        P(("dom", "sub")),
    )
    return jax.shard_map(
        shards,
        mesh=mesh,
        in_specs=placed,
        out_specs=(P(None, "dom"), P(("dom", "sub"))),
        check_vma=False,
    )
```

```python
import functools

import jax
import jax.numpy as jnp
from jax import lax
from jax.experimental import pallas as pl
from jax.experimental.pallas import tpu as pltpu
from jax.sharding import PartitionSpec as P

ORDER = 8
LANES = 128


precise = lax.Precision.HIGHEST


def round_up(count, unit):
    return -(-count // unit) * unit


def exponents():
    entries = []
    for degree in range(ORDER + 1):
        for along_x in range(degree, -1, -1):
            for along_y in range(degree - along_x, -1, -1):
                entries.append((along_x, along_y, degree - along_x - along_y))
    return entries


def halves(value):
    high = value.astype(jnp.bfloat16)
    low = (value - high.astype(jnp.float32)).astype(jnp.bfloat16)
    return high, low


def one_hot(row, count):
    places = lax.broadcasted_iota(jnp.int32, (count, row.shape[1]), 0)
    return jnp.where(places == row, 1.0, 0.0).astype(jnp.bfloat16)


def interact_kernel(
    coeffs, slots, group, spread, tops, fine_ref, tops_ref, upward_ref, fine_list, coarse_list,
    ops_ref, out_ref,
    fine_table, coarse_table, fine_picked, coarse_picked, held,
):
    rows = fine_ref.shape[0]
    depth = fine_list.shape[0]
    step = pl.program_id(0)

    @pl.when(step == 0)
    def _():
        ops_high, ops_low = split_upward(upward_ref, held)
        width = coarse_table.shape[1]

        def shifted(value, amount):
            extra = width - value.shape[1]
            if extra:
                filler = jnp.zeros((rows, extra), jnp.float32)
                value = jnp.concatenate([value, filler], axis=1)
            return pltpu.roll(value, amount, 1) if amount else value

        top_moments = jnp.transpose(tops_ref[...])[:rows]
        coarse = shifted(raise_level(fine_ref[...], ops_high, ops_low), 0)
        coarse += shifted(top_moments, spread)
        coarse += shifted(raise_level(top_moments, ops_high, ops_low), spread + tops)
        for source, table in ((fine_ref[...], fine_table), (coarse, coarse_table)):
            high, low = halves(source)
            table[...] = jnp.concatenate([high, low], axis=0)

        def pick(batch, carry):
            base = pl.multiple_of(8 * batch, 8)
            for table, entries, picked in (
                (fine_table, fine_list, fine_picked),
                (coarse_table, coarse_list, coarse_picked),
            ):
                columns = []
                for k in range(0, 8, 2):
                    chosen = jnp.concatenate(
                        [
                            one_hot(entries[pl.ds(base + k + m, 1), :], table.shape[1])
                            for m in range(2)
                        ],
                        axis=1,
                    )
                    both = jnp.dot(table[...], chosen, preferred_element_type=jnp.float32)
                    value = both[:rows] + both[rows:]
                    columns += [value[:, :LANES], value[:, LANES:]]
                picked[:, pl.ds(base, 8), :] = jnp.swapaxes(jnp.stack(columns), 0, 1)
            return carry

        lax.fori_loop(0, depth // 8, pick, 0)
        out_ref[...] = jnp.zeros_like(out_ref)

    lane = lax.broadcasted_iota(jnp.int32, (rows, LANES), 1)
    filler = jnp.zeros((LANES - depth, 2 * LANES), jnp.bfloat16)
    for part in range(group // 8):
        block = jnp.swapaxes(ops_ref[:, 8 * part : 8 * part + 8, :], 0, 1)
        left = []
        right = []
        for k in range(8):
            term = step * group + 8 * part + k
            op = jnp.where((lane < slots) & (term < coeffs), block[k], 0.0)
            op_high, op_low = halves(op)
            data = jnp.concatenate([fine_picked[term], coarse_picked[term]], axis=1)
            high, low = halves(data)
            high = jnp.concatenate([high, filler], axis=0)
            low = jnp.concatenate([low, filler], axis=0)
            left += [op_high, op_high, op_low]
            right += [high, low, high]
        out_ref[...] += jnp.dot(
            jnp.concatenate(left, axis=1),
            jnp.concatenate(right, axis=0),
            preferred_element_type=jnp.float32,
        )


def interact(fine, tops_rows, upward_ops, fine_list, coarse_list, ops, spread, tops, coarse_width):
    coeffs, _, slots = ops.shape
    rows, width = fine.shape
    depth = fine_list.shape[0]
    group = 24
    whole = lambda array: pl.BlockSpec(array.shape, lambda i: (0, 0))
    return pl.pallas_call(
        functools.partial(interact_kernel, coeffs, slots, group, spread, tops),
        grid=(rows // group,),
        in_specs=[
            whole(fine),
            whole(tops_rows),
            pl.BlockSpec((coeffs, 8, coeffs), lambda i: (0, 0, 0)),
            whole(fine_list),
            whole(coarse_list),
            pl.BlockSpec((rows, group, LANES), lambda i: (0, i, 0)),
        ],
        out_specs=pl.BlockSpec((rows, 2 * LANES), lambda i: (0, 0)),
        out_shape=jax.ShapeDtypeStruct((rows, 2 * LANES), jnp.float32),
        scratch_shapes=[
            pltpu.VMEM((2 * rows, width), jnp.bfloat16),
            pltpu.VMEM((2 * rows, coarse_width), jnp.bfloat16),
            pltpu.VMEM((rows, depth, LANES), jnp.float32),
            pltpu.VMEM((rows, depth, LANES), jnp.float32),
            pltpu.VMEM((rows, 8, 2 * LANES), jnp.float32),
        ],
        compiler_params=pltpu.CompilerParams(vmem_limit_bytes=48 * 1024 * 1024),
        cost_estimate=pl.CostEstimate(
            flops=6 * rows * rows * LANES * 2 * LANES,
            bytes_accessed=4 * rows * rows * LANES,
            transcendentals=0,
        ),
    )(fine, tops_rows, jnp.transpose(upward_ops, (1, 0, 2)), fine_list, coarse_list, ops)


def potential_kernel(local_ref, leaf_ref, position_ref, exponent_ref, out_ref):
    rows, cells = local_ref.shape
    particles = leaf_ref.shape[1]
    high, low = halves(local_ref[...])
    table = jnp.concatenate([high, low], axis=0)
    masks = [
        [(exponent_ref[:, axis : axis + 1] // bit) % 2 == 1 for bit in (1, 2, 4, 8)]
        for axis in range(3)
    ]
    for start in range(0, particles, 2 * LANES):
        span = slice(start, start + 2 * LANES)
        chosen = one_hot(leaf_ref[:, span], cells)
        both = jnp.dot(table, chosen, preferred_element_type=jnp.float32)
        value = both[:rows] + both[rows:]
        for axis in range(3):
            power = position_ref[axis : axis + 1, span]
            for bit in range(4):
                value = value * jnp.where(masks[axis][bit], power, 1.0)
                power = power * power
        out_ref[:, span] = jnp.sum(value, axis=0, keepdims=True)


def evaluate(local, leaves, positions):
    rows = local.shape[0]
    table = jnp.asarray(exponents(), jnp.int32)
    table = jnp.pad(table, ((0, rows - table.shape[0]), (0, LANES - 3)))
    return pl.pallas_call(
        potential_kernel,
        out_shape=jax.ShapeDtypeStruct((1, leaves.shape[0]), jnp.float32),
        compiler_params=pltpu.CompilerParams(vmem_limit_bytes=32 * 1024 * 1024),
    )(local, leaves[None], positions, table)[0]


def raise_level(moments, ops_high, ops_low):
    rows, width = moments.shape
    parents = round_up(width // 8, LANES)
    high, low = halves(moments)
    source = lax.broadcasted_iota(jnp.int32, (width, 8 * parents), 0)
    target = lax.broadcasted_iota(jnp.int32, (width, 8 * parents), 1)
    wanted = 8 * (target % parents) + target // parents
    chosen = jnp.where(source == wanted, 1.0, 0.0).astype(jnp.bfloat16)
    both = jnp.dot(
        jnp.concatenate([high, low], axis=0), chosen, preferred_element_type=jnp.float32
    )
    filler = jnp.zeros((2 * LANES - rows, parents), jnp.float32)
    stacks = []
    for first in (0, rows):
        pieces = []
        for o in range(8):
            pieces += [both[first : first + rows, o * parents : (o + 1) * parents], filler]
        stacks.append(jnp.concatenate(pieces, axis=0).astype(jnp.bfloat16))
    dot = functools.partial(jnp.dot, preferred_element_type=jnp.float32)
    return dot(ops_high, stacks[0]) + dot(ops_high, stacks[1]) + dot(ops_low, stacks[0])


def split_upward(upward_ref, held):
    coeffs = upward_ref.shape[0]
    held[...] = jnp.zeros_like(held)
    held[:coeffs, :, :coeffs] = upward_ref[...]
    ops = jnp.swapaxes(held[...], 0, 1)
    return halves(jnp.concatenate([ops[o] for o in range(8)], axis=1))


def prepare_kernel(
    counts, partial_ref, upward_ref, fine_ref, mid_ref, top_ref, upper_ref,
    block_out, rows_out, fine_out, coarse_out, held, lists,
):
    rows = block_out.shape[0]
    coeffs = partial_ref.shape[0]
    slots = fine_ref.shape[0]
    slab, mid, top, spread, tops = counts
    domain = lax.axis_index("dom")
    block_out[...] = jnp.zeros_like(block_out)
    block_out[:coeffs, :] = partial_ref[...]
    high, low = split_upward(upward_ref, held)
    top_moments = raise_level(raise_level(block_out[...], high, low), high, low)
    filler = jnp.zeros((2 * LANES - rows, LANES), jnp.float32)
    turned = jnp.transpose(jnp.concatenate([top_moments, filler], axis=0))
    rows_out[...] = turned[: rows_out.shape[0]]

    def place(sources, offset):
        return jnp.where(sources >= 0, sources + offset, -1)

    fine_out[...] = jnp.full_like(fine_out, -1)
    fine_out[:slots, :] = place(fine_ref[...], slab - domain * slab)
    lists[...] = jnp.full_like(lists, -1.0)
    start = 0
    for part in (
        place(mid_ref[...], mid - domain * mid),
        place(top_ref[...], spread),
        place(upper_ref[pl.ds(domain * top // 8, 1), :], spread + tops),
    ):
        lists[start : start + part.shape[0], :slots] = part.astype(jnp.float32)
        start += part.shape[0]
    coarse = jnp.transpose(lists[...])
    coarse_out[...] = coarse[: coarse_out.shape[0]].astype(jnp.int32)


def exchange_kernel(
    domains, subs, block_ref, top_ref, wide_out, tops_out,
    sides, tops, side_send, side_recv, top_send, top_recv, own_sem,
):
    domain, sub = lax.axis_index("dom"), lax.axis_index("sub")
    count = domains * subs
    flat = domain * subs + sub
    mesh = pl.DeviceIdType.MESH
    cells = block_ref.shape[1]
    top_cells = top_ref.shape[0]

    def peer(offset):
        place = lax.rem(flat + offset, count)
        return {"dom": place // subs, "sub": lax.rem(place, subs)}

    barrier = pltpu.get_barrier_semaphore()

    def greet(offset, carry):
        pl.semaphore_signal(barrier, inc=1, device_id=peer(offset), device_id_type=mesh)
        return carry

    lax.fori_loop(1, count, greet, 0)
    own = pltpu.make_async_copy(top_ref, tops.at[count - 1], own_sem)
    own.start()
    pl.semaphore_wait(barrier, count - 1)
    copies = []
    for turn in range(subs):
        for index, move in enumerate((1, domains - 1, 0)):
            if turn == 0 and move == 0:
                continue
            side = pltpu.make_async_remote_copy(
                src_ref=block_ref,
                dst_ref=sides.at[index, turn],
                send_sem=side_send.at[index, turn],
                recv_sem=side_recv.at[index, turn],
                device_id={
                    "dom": lax.rem(domain + move, domains),
                    "sub": lax.rem(sub + turn, subs),
                },
                device_id_type=mesh,
            )
            side.start()
            copies.append(side)

    def send(offset, carry):
        pltpu.make_async_remote_copy(
            src_ref=top_ref,
            dst_ref=tops.at[offset - 1],
            send_sem=top_send,
            recv_sem=top_recv,
            device_id=peer(offset),
            device_id_type=mesh,
        ).start()
        return carry

    lax.fori_loop(1, count, send, 0)
    own.wait()
    arrived = tops.at[pl.ds(0, count - 1)]
    pltpu.make_async_copy(arrived, arrived, top_recv).wait()
    tops_out[...] = jnp.zeros_like(tops_out)

    def gather(offset, carry):
        source = lax.rem(flat + count - offset, count) // subs
        slot = lax.rem(offset + count - 1, count)
        for r in range(top_cells):
            at = pl.ds(source * top_cells + r, 1)
            tops_out[at, :] = tops_out[at, :] + tops[slot, r : r + 1, :]
        return carry

    lax.fori_loop(0, count, gather, 0)
    for side in copies:
        side.wait()
    for index, start in ((0, 0), (2, cells), (1, 2 * cells)):
        held = [block_ref[...]] if index == 2 else [sides[index, 0]]
        for turn in range(1, subs):
            held.append(sides[index, turn])
        wide_out[:, start : start + cells] = sum(held[1:], held[0])
    pltpu.make_async_copy(arrived, arrived, top_send).wait()


def exchange(block, top_rows, coarse_tops):
    domains, subs = lax.axis_size("dom"), lax.axis_size("sub")
    vmem = pl.BlockSpec(memory_space=pltpu.VMEM)
    rows, cells = block.shape
    return pl.pallas_call(
        functools.partial(exchange_kernel, domains, subs),
        in_specs=[vmem, vmem],
        out_specs=[vmem] * 2,
        out_shape=[
            jax.ShapeDtypeStruct((rows, 3 * cells), jnp.float32),
            jax.ShapeDtypeStruct((coarse_tops, top_rows.shape[1]), jnp.float32),
        ],
        scratch_shapes=[
            pltpu.VMEM((3, subs) + block.shape, jnp.float32),
            pltpu.VMEM((domains * subs,) + top_rows.shape, jnp.float32),
            pltpu.SemaphoreType.DMA((3, subs)),
            pltpu.SemaphoreType.DMA((3, subs)),
            pltpu.SemaphoreType.DMA,
            pltpu.SemaphoreType.DMA,
            pltpu.SemaphoreType.DMA,
        ],
        compiler_params=pltpu.CompilerParams(collective_id=0, has_side_effects=True),
    )(block, top_rows)


def prepare(partial, upward_ops, fine_list, mid_list, top_list, upper_list, rows, depth, counts):
    coeffs, cells = partial.shape
    top_cells = top_list.shape[1]
    vmem = pl.BlockSpec(memory_space=pltpu.VMEM)

    return pl.pallas_call(
        functools.partial(prepare_kernel, counts),
        in_specs=[vmem] * 6,
        out_specs=[vmem] * 4,
        out_shape=[
            jax.ShapeDtypeStruct((rows, cells), jnp.float32),
            jax.ShapeDtypeStruct((top_cells, 2 * LANES), jnp.float32),
            jax.ShapeDtypeStruct((depth, LANES), jnp.int32),
            jax.ShapeDtypeStruct((depth, LANES), jnp.int32),
        ],
        scratch_shapes=[
            pltpu.VMEM((rows, 8, 2 * LANES), jnp.float32),
            pltpu.VMEM((LANES, LANES), jnp.float32),
        ],
        compiler_params=pltpu.CompilerParams(vmem_limit_bytes=32 * 1024 * 1024),
    )(
        partial,
        jnp.transpose(upward_ops, (1, 0, 2)),
        fine_list,
        jnp.transpose(mid_list),
        jnp.transpose(top_list),
        jnp.transpose(upper_list),
    )


def downward(expansions, downward_ops):
    spread = jnp.einsum("oab,bp->apo", downward_ops, expansions, precision=precise)
    return spread.reshape(spread.shape[0], -1)


def settle(portion):
    count = lax.axis_size("sub")
    ring = [(i, (i + 1) % count) for i in range(count)]
    total = moving = portion
    for _ in range(count - 1):
        moving = lax.ppermute(moving, "sub", ring)
        total = total + moving
    return total


def shards(
    fine_partial,
    upward_ops,
    interaction_ops,
    downward_ops,
    fine_list,
    mid_list,
    top_list,
    upper_list,
    positions,
    leaf_cell,
):
    slab_cells = fine_partial.shape[2]
    mid_cells = slab_cells // 8
    top_cells = slab_cells // 64
    domain = lax.axis_index("dom")
    slots, coeffs = interaction_ops.shape[:2]
    rows = round_up(coeffs, 24)
    depth = round_up(slots, 16)
    upper_span = max(1, top_cells // 8)
    spread = 3 * mid_cells
    tops = top_cells * lax.axis_size("dom")
    coarse_width = round_up(spread + tops + tops // 8, LANES)
    counts = (slab_cells, mid_cells, top_cells, spread, tops)
    block, top_rows, fine_sources, coarse_sources = prepare(
        fine_partial[0], upward_ops, fine_list, mid_list, top_list, upper_list,
        rows, depth, counts,
    )
    wide_fine, top_moments = exchange(block, top_rows, round_up(tops, LANES))

    def padded(array, height, width, fill):
        return jnp.pad(
            array,
            ((0, height - array.shape[0]), (0, width - array.shape[1])),
            constant_values=fill,
        )

    terms = interact(
        wide_fine, top_moments, upward_ops, fine_sources, coarse_sources,
        jnp.transpose(interaction_ops, (1, 2, 0)), spread, tops, coarse_width,
    )
    terms = settle(terms)[:coeffs]
    at = LANES
    mid_term = terms[:, at : at + mid_cells]
    at += mid_cells
    top_term = terms[:, at : at + top_cells]
    at += top_cells
    local_upper = terms[:, at : at + upper_span]
    down_top = downward(local_upper, downward_ops)
    top_offset = domain * top_cells % 8
    local_top = top_term + lax.dynamic_slice_in_dim(down_top, top_offset, top_cells, 1)
    local_mid = mid_term + downward(local_top, downward_ops)
    local_fine = terms[:, :slab_cells] + downward(local_mid, downward_ops)
    potential = evaluate(
        padded(local_fine, rows, slab_cells, 0), leaf_cell - domain * slab_cells, positions
    )
    return (local_fine, potential)


def solution(mesh):
    placed = (
        P("sub", None, "dom"),
        P(),
        P("sub", None, None),
        P(),
        P("sub", "dom"),
        P("sub", "dom"),
        P("sub", "dom"),
        P("sub", None),
        P(None, ("dom", "sub")),
        P(("dom", "sub")),
    )
    return jax.shard_map(
        shards,
        mesh=mesh,
        in_specs=placed,
        out_specs=(P(None, "dom"), P(("dom", "sub"))),
        check_vma=False,
    )
```

```python
import functools

import jax
import jax.numpy as jnp
from jax import lax
from jax.experimental import pallas as pl
from jax.experimental.pallas import tpu as pltpu
from jax.sharding import PartitionSpec as P

ORDER = 8
LANES = 128


precise = lax.Precision.HIGHEST


def round_up(count, unit):
    return -(-count // unit) * unit


def exponents():
    entries = []
    for degree in range(ORDER + 1):
        for along_x in range(degree, -1, -1):
            for along_y in range(degree - along_x, -1, -1):
                entries.append((along_x, along_y, degree - along_x - along_y))
    return entries


def halves(value):
    high = value.astype(jnp.bfloat16)
    low = (value - high.astype(jnp.float32)).astype(jnp.bfloat16)
    return high, low


def one_hot(row, count):
    places = lax.broadcasted_iota(jnp.int32, (count, row.shape[1]), 0)
    return jnp.where(places == row, 1.0, 0.0).astype(jnp.bfloat16)


def interact_kernel(
    coeffs, slots, group, spread, tops, fine_ref, tops_ref, upward_ref, fine_list, coarse_list,
    ops_ref, out_ref,
    fine_table, coarse_table, fine_picked, coarse_picked, held,
):
    rows = fine_ref.shape[0]
    depth = fine_list.shape[0]
    step = pl.program_id(0)

    @pl.when(step == 0)
    def _():
        ops_high, ops_low = split_upward(upward_ref, held)
        width = coarse_table.shape[1]

        def shifted(value, amount):
            extra = width - value.shape[1]
            if extra:
                filler = jnp.zeros((rows, extra), jnp.float32)
                value = jnp.concatenate([value, filler], axis=1)
            return pltpu.roll(value, amount, 1) if amount else value

        top_moments = jnp.transpose(tops_ref[...])[:rows]
        coarse = shifted(raise_level(fine_ref[...], ops_high, ops_low), 0)
        coarse += shifted(top_moments, spread)
        coarse += shifted(raise_level(top_moments, ops_high, ops_low), spread + tops)
        for source, table in ((fine_ref[...], fine_table), (coarse, coarse_table)):
            high, low = halves(source)
            table[...] = jnp.concatenate([high, low], axis=0)

        def pick(batch, carry):
            base = pl.multiple_of(8 * batch, 8)
            for table, entries, picked in (
                (fine_table, fine_list, fine_picked),
                (coarse_table, coarse_list, coarse_picked),
            ):
                columns = []
                for k in range(0, 8, 2):
                    chosen = jnp.concatenate(
                        [
                            one_hot(entries[pl.ds(base + k + m, 1), :], table.shape[1])
                            for m in range(2)
                        ],
                        axis=1,
                    )
                    both = jnp.dot(table[...], chosen, preferred_element_type=jnp.float32)
                    value = both[:rows] + both[rows:]
                    columns += [value[:, :LANES], value[:, LANES:]]
                picked[:, pl.ds(base, 8), :] = jnp.swapaxes(jnp.stack(columns), 0, 1)
            return carry

        lax.fori_loop(0, depth // 8, pick, 0)
        out_ref[...] = jnp.zeros_like(out_ref)

    lane = lax.broadcasted_iota(jnp.int32, (rows, LANES), 1)
    filler = jnp.zeros((LANES - depth, 2 * LANES), jnp.bfloat16)
    for part in range(group // 8):
        block = jnp.swapaxes(ops_ref[:, 8 * part : 8 * part + 8, :], 0, 1)
        left = []
        right = []
        for k in range(8):
            term = step * group + 8 * part + k
            op = jnp.where((lane < slots) & (term < coeffs), block[k], 0.0)
            op_high, op_low = halves(op)
            data = jnp.concatenate([fine_picked[term], coarse_picked[term]], axis=1)
            high, low = halves(data)
            high = jnp.concatenate([high, filler], axis=0)
            low = jnp.concatenate([low, filler], axis=0)
            left += [op_high, op_high, op_low]
            right += [high, low, high]
        out_ref[...] += jnp.dot(
            jnp.concatenate(left, axis=1),
            jnp.concatenate(right, axis=0),
            preferred_element_type=jnp.float32,
        )


def interact(fine, tops_rows, upward_ops, fine_list, coarse_list, ops, spread, tops, coarse_width):
    coeffs, _, slots = ops.shape
    rows, width = fine.shape
    depth = fine_list.shape[0]
    group = 24
    whole = lambda array: pl.BlockSpec(array.shape, lambda i: (0, 0))
    return pl.pallas_call(
        functools.partial(interact_kernel, coeffs, slots, group, spread, tops),
        grid=(rows // group,),
        in_specs=[
            whole(fine),
            whole(tops_rows),
            pl.BlockSpec((coeffs, 8, coeffs), lambda i: (0, 0, 0)),
            whole(fine_list),
            whole(coarse_list),
            pl.BlockSpec((rows, group, LANES), lambda i: (0, i, 0)),
        ],
        out_specs=pl.BlockSpec((rows, 2 * LANES), lambda i: (0, 0)),
        out_shape=jax.ShapeDtypeStruct((rows, 2 * LANES), jnp.float32),
        scratch_shapes=[
            pltpu.VMEM((2 * rows, width), jnp.bfloat16),
            pltpu.VMEM((2 * rows, coarse_width), jnp.bfloat16),
            pltpu.VMEM((rows, depth, LANES), jnp.float32),
            pltpu.VMEM((rows, depth, LANES), jnp.float32),
            pltpu.VMEM((rows, 8, 2 * LANES), jnp.float32),
        ],
        compiler_params=pltpu.CompilerParams(vmem_limit_bytes=48 * 1024 * 1024),
        cost_estimate=pl.CostEstimate(
            flops=6 * rows * rows * LANES * 2 * LANES,
            bytes_accessed=4 * rows * rows * LANES,
            transcendentals=0,
        ),
    )(fine, tops_rows, jnp.transpose(upward_ops, (1, 0, 2)), fine_list, coarse_list, ops)


def potential_kernel(local_ref, leaf_ref, position_ref, exponent_ref, out_ref):
    rows, cells = local_ref.shape
    particles = leaf_ref.shape[1]
    high, low = halves(local_ref[...])
    table = jnp.concatenate([high, low], axis=0)
    masks = [
        [(exponent_ref[:, axis : axis + 1] // bit) % 2 == 1 for bit in (1, 2, 4, 8)]
        for axis in range(3)
    ]
    for start in range(0, particles, 2 * LANES):
        span = slice(start, start + 2 * LANES)
        chosen = one_hot(leaf_ref[:, span], cells)
        both = jnp.dot(table, chosen, preferred_element_type=jnp.float32)
        value = both[:rows] + both[rows:]
        for axis in range(3):
            power = position_ref[axis : axis + 1, span]
            for bit in range(4):
                value = value * jnp.where(masks[axis][bit], power, 1.0)
                power = power * power
        out_ref[:, span] = jnp.sum(value, axis=0, keepdims=True)


def evaluate(local, leaves, positions):
    rows = local.shape[0]
    table = jnp.asarray(exponents(), jnp.int32)
    table = jnp.pad(table, ((0, rows - table.shape[0]), (0, LANES - 3)))
    return pl.pallas_call(
        potential_kernel,
        out_shape=jax.ShapeDtypeStruct((1, leaves.shape[0]), jnp.float32),
        compiler_params=pltpu.CompilerParams(vmem_limit_bytes=32 * 1024 * 1024),
    )(local, leaves[None], positions, table)[0]


def raise_level(moments, ops_high, ops_low):
    rows, width = moments.shape
    parents = round_up(width // 8, LANES)
    high, low = halves(moments)
    source = lax.broadcasted_iota(jnp.int32, (width, 8 * parents), 0)
    target = lax.broadcasted_iota(jnp.int32, (width, 8 * parents), 1)
    wanted = 8 * (target % parents) + target // parents
    chosen = jnp.where(source == wanted, 1.0, 0.0).astype(jnp.bfloat16)
    both = jnp.dot(
        jnp.concatenate([high, low], axis=0), chosen, preferred_element_type=jnp.float32
    )
    filler = jnp.zeros((2 * LANES - rows, parents), jnp.float32)
    stacks = []
    for first in (0, rows):
        pieces = []
        for o in range(8):
            pieces += [both[first : first + rows, o * parents : (o + 1) * parents], filler]
        stacks.append(jnp.concatenate(pieces, axis=0).astype(jnp.bfloat16))
    dot = functools.partial(jnp.dot, preferred_element_type=jnp.float32)
    return dot(ops_high, stacks[0]) + dot(ops_high, stacks[1]) + dot(ops_low, stacks[0])


def split_upward(upward_ref, held):
    coeffs = upward_ref.shape[0]
    held[...] = jnp.zeros_like(held)
    held[:coeffs, :, :coeffs] = upward_ref[...]
    ops = jnp.swapaxes(held[...], 0, 1)
    return halves(jnp.concatenate([ops[o] for o in range(8)], axis=1))


def prepare(
    counts, partial_ref, upward_ref, fine_ref, mid_ref, top_ref, upper_ref,
    rows_out, fine_out, coarse_out, held, lists,
):
    rows = held.shape[0]
    coeffs = partial_ref.shape[0]
    slots = fine_ref.shape[0]
    slab, mid, top, spread, tops = counts
    domain = lax.axis_index("dom")
    filler = jnp.zeros((rows - coeffs, partial_ref.shape[1]), jnp.float32)
    block = jnp.concatenate([partial_ref[...], filler], axis=0)
    high, low = split_upward(upward_ref, held)
    top_moments = raise_level(raise_level(block, high, low), high, low)
    filler = jnp.zeros((2 * LANES - rows, LANES), jnp.float32)
    turned = jnp.transpose(jnp.concatenate([top_moments, filler], axis=0))
    rows_out[...] = turned[: rows_out.shape[0]]

    def place(sources, offset):
        return jnp.where(sources >= 0, sources + offset, -1)

    fine_out[...] = jnp.full_like(fine_out, -1)
    fine_out[:slots, :] = place(fine_ref[...], slab - domain * slab)
    lists[...] = jnp.full_like(lists, -1.0)
    start = 0
    for part in (
        place(mid_ref[...], mid - domain * mid),
        place(top_ref[...], spread),
        place(upper_ref[pl.ds(domain * top // 8, 1), :], spread + tops),
    ):
        lists[start : start + part.shape[0], :slots] = part.astype(jnp.float32)
        start += part.shape[0]
    coarse = jnp.transpose(lists[...])
    coarse_out[...] = coarse[: coarse_out.shape[0]].astype(jnp.int32)


def exchange_kernel(
    domains, subs, counts, block_ref, partial_ref, upward_ref, fine_ref, mid_ref, top_list_ref,
    upper_ref, wide_out, tops_out, fine_out, coarse_out,
    low, high, tops, top_ref, held, lists, side_send, side_recv, top_send, top_recv,
):
    domain, sub = lax.axis_index("dom"), lax.axis_index("sub")
    count = domains * subs
    flat = domain * subs + sub
    mesh = pl.DeviceIdType.MESH
    coeffs, cells = block_ref.shape
    top_cells = top_ref.shape[0]

    def peer(offset):
        place = lax.rem(flat + offset, count)
        return {"dom": place // subs, "sub": lax.rem(place, subs)}

    barrier = pltpu.get_barrier_semaphore()

    def greet(offset, carry):
        pl.semaphore_signal(barrier, inc=1, device_id=peer(offset), device_id_type=mesh)
        return carry

    lax.fori_loop(1, count, greet, 0)
    prepare(
        counts, partial_ref, upward_ref, fine_ref, mid_ref, top_list_ref, upper_ref,
        top_ref, fine_out, coarse_out, held, lists,
    )
    tops[count - 1] = top_ref[...]
    tops_out[...] = jnp.zeros_like(tops_out)
    wide_out[...] = jnp.zeros_like(wide_out)
    wide_out[:coeffs, cells : 2 * cells] = block_ref[...]
    pl.semaphore_wait(barrier, count - 1)

    def send(offset, carry):
        pltpu.make_async_remote_copy(
            src_ref=top_ref,
            dst_ref=tops.at[offset - 1],
            send_sem=top_send,
            recv_sem=top_recv,
            device_id=peer(offset),
            device_id_type=mesh,
        ).start()
        return carry

    lax.fori_loop(1, count, send, 0)
    copies = []
    for index, (target, move) in enumerate(((low, 1), (high, domains - 1))):
        side = pltpu.make_async_remote_copy(
            src_ref=block_ref,
            dst_ref=target,
            send_sem=side_send.at[index],
            recv_sem=side_recv.at[index],
            device_id={"dom": lax.rem(domain + move, domains), "sub": sub},
            device_id_type=mesh,
        )
        side.start()
        copies.append(side)
    arrived = tops.at[pl.ds(0, count - 1)]
    pltpu.make_async_copy(arrived, arrived, top_recv).wait()

    def gather(offset, carry):
        source = lax.rem(flat + count - offset, count) // subs
        slot = lax.rem(offset + count - 1, count)
        for r in range(top_cells):
            at = pl.ds(source * top_cells + r, 1)
            tops_out[at, :] = tops_out[at, :] + tops[slot, r : r + 1, :]
        return carry

    lax.fori_loop(0, count, gather, 0)
    for side in copies:
        side.wait()
    wide_out[:coeffs, :cells] = low[...]
    wide_out[:coeffs, 2 * cells :] = high[...]
    pltpu.make_async_copy(arrived, arrived, top_send).wait()


def exchange(block, partial, upward_ops, fine_list, mid_list, top_list, upper_list, rows, depth, counts):
    domains, subs = lax.axis_size("dom"), lax.axis_size("sub")
    coeffs, cells = block.shape
    top_cells = top_list.shape[1]
    vmem = pl.BlockSpec(memory_space=pltpu.VMEM)
    return pl.pallas_call(
        functools.partial(exchange_kernel, domains, subs, counts),
        in_specs=[vmem] * 7,
        out_specs=[vmem] * 4,
        out_shape=[
            jax.ShapeDtypeStruct((rows, 3 * cells), jnp.float32),
            jax.ShapeDtypeStruct((round_up(counts[4], LANES), 2 * LANES), jnp.float32),
            jax.ShapeDtypeStruct((depth, LANES), jnp.int32),
            jax.ShapeDtypeStruct((depth, LANES), jnp.int32),
        ],
        scratch_shapes=[
            pltpu.VMEM(block.shape, jnp.float32),
            pltpu.VMEM(block.shape, jnp.float32),
            pltpu.VMEM((domains * subs, top_cells, 2 * LANES), jnp.float32),
            pltpu.VMEM((top_cells, 2 * LANES), jnp.float32),
            pltpu.VMEM((rows, 8, 2 * LANES), jnp.float32),
            pltpu.VMEM((LANES, LANES), jnp.float32),
            pltpu.SemaphoreType.DMA((2,)),
            pltpu.SemaphoreType.DMA((2,)),
            pltpu.SemaphoreType.DMA,
            pltpu.SemaphoreType.DMA,
        ],
        compiler_params=pltpu.CompilerParams(
            collective_id=0, has_side_effects=True, vmem_limit_bytes=32 * 1024 * 1024
        ),
    )(
        block,
        partial,
        jnp.transpose(upward_ops, (1, 0, 2)),
        fine_list,
        jnp.transpose(mid_list),
        jnp.transpose(top_list),
        jnp.transpose(upper_list),
    )


def downward(expansions, downward_ops):
    spread = jnp.einsum("oab,bp->apo", downward_ops, expansions, precision=precise)
    return spread.reshape(spread.shape[0], -1)


def settle(portion):
    count = lax.axis_size("sub")
    ring = [(i, (i + 1) % count) for i in range(count)]
    total = moving = portion
    for _ in range(count - 1):
        moving = lax.ppermute(moving, "sub", ring)
        total = total + moving
    return total


def shards(
    fine_partial,
    upward_ops,
    interaction_ops,
    downward_ops,
    fine_list,
    mid_list,
    top_list,
    upper_list,
    positions,
    leaf_cell,
):
    slab_cells = fine_partial.shape[2]
    mid_cells = slab_cells // 8
    top_cells = slab_cells // 64
    domain = lax.axis_index("dom")
    slots, coeffs = interaction_ops.shape[:2]
    rows = round_up(coeffs, 24)
    depth = round_up(slots, 16)
    upper_span = max(1, top_cells // 8)
    spread = 3 * mid_cells
    tops = top_cells * lax.axis_size("dom")
    coarse_width = round_up(spread + tops + tops // 8, LANES)
    counts = (slab_cells, mid_cells, top_cells, spread, tops)
    partial = fine_partial[0]
    wide_fine, top_moments, fine_sources, coarse_sources = exchange(
        settle(partial), partial, upward_ops, fine_list, mid_list, top_list, upper_list,
        rows, depth, counts,
    )

    def padded(array, height, width, fill):
        return jnp.pad(
            array,
            ((0, height - array.shape[0]), (0, width - array.shape[1])),
            constant_values=fill,
        )

    terms = interact(
        wide_fine, top_moments, upward_ops, fine_sources, coarse_sources,
        jnp.transpose(interaction_ops, (1, 2, 0)), spread, tops, coarse_width,
    )
    terms = settle(terms)[:coeffs]
    at = LANES
    mid_term = terms[:, at : at + mid_cells]
    at += mid_cells
    top_term = terms[:, at : at + top_cells]
    at += top_cells
    local_upper = terms[:, at : at + upper_span]
    down_top = downward(local_upper, downward_ops)
    top_offset = domain * top_cells % 8
    local_top = top_term + lax.dynamic_slice_in_dim(down_top, top_offset, top_cells, 1)
    local_mid = mid_term + downward(local_top, downward_ops)
    local_fine = terms[:, :slab_cells] + downward(local_mid, downward_ops)
    potential = evaluate(
        padded(local_fine, rows, slab_cells, 0), leaf_cell - domain * slab_cells, positions
    )
    return (local_fine, potential)


def solution(mesh):
    placed = (
        P("sub", None, "dom"),
        P(),
        P("sub", None, None),
        P(),
        P("sub", "dom"),
        P("sub", "dom"),
        P("sub", "dom"),
        P("sub", None),
        P(None, ("dom", "sub")),
        P(("dom", "sub")),
    )
    return jax.shard_map(
        shards,
        mesh=mesh,
        in_specs=placed,
        out_specs=(P(None, "dom"), P(("dom", "sub"))),
        check_vma=False,
    )
```
